32 devices in a mesh: row: 8 (over z, y), col: 4 (over x, core).
Axes of the slice: x: 2, y: 2, z: 4, core: 2. Of those that a mesh axis runs over, the one named last changes fastest.
Arguments:
- acts_in: bfloat16 [8192, 4608], P('row'), may hold values from -64 to 64
- grad_query: bfloat16 [8192, 4096], P('row', 'col'), may hold values from -2.828427 to 2.828427
- attn_out: bfloat16 [8192, 4096], P('row'), may hold values from -64 to 64
- grad_out: bfloat16 [8192, 4608], P('row', 'col'), may hold values from -2.828427 to 2.828427
- row_query: float32 [4608], P('row'), may hold values from 0.05 to 18
- col_query: float32 [4096], P('col'), may hold values from 0.05 to 2
- row_output: float32 [4096], P('row'), may hold values from 0.05 to 18
- col_output: float32 [4608], P('col'), may hold values from 0.05 to 2
Outputs:
- update_query: bfloat16 [4608, 4096], P('row', 'col')
- update_output: bfloat16 [4096, 4608], P('row', 'col')
- new_row_query: float32 [4608], P('row')
- new_col_query: float32 [4096], P('col')
- new_row_output: float32 [4096], P('row')
- new_col_output: float32 [4608], P('col')
The draws below stay inside these ranges and needn't reach their ends.
All inputs are finite; a program needn't handle non-finite values.
Results may differ from the reference program's by a relative error of at most 0.028.
Values may be sent and summed in bfloat16 or wider, within the bound.
A program may use at most 128 MiB of HBM per device.

```python
import math
import jax
import jax.numpy as jnp
from jax import lax

D = 4608
Q = 4096
TOK_DEV = 1024
CLIP = 3072
TOKENS = 8192
N_ROW = 8


def scaled_field(key, row_count, col_count, size_scale):
    key_list = jax.random.split(key, 2)
    col_scale = jnp.exp(jax.random.uniform(key_list[1], (col_count,), jnp.float32, 0.0, math.log(10.0)))
    col_scale = col_scale * jnp.exp(math.log(3.0) * jnp.arange(col_count, dtype=jnp.float32) / col_count)
    col_scale = col_scale / jnp.sqrt(jnp.mean(col_scale * col_scale))
    base_field = jax.random.normal(key_list[0], (row_count, col_count), jnp.float32)
    field_bound = 64.0 * size_scale
    return jnp.clip(base_field * col_scale * size_scale, -field_bound, field_bound).astype(jnp.bfloat16)


def rising_factor(key, count):
    base_value = jnp.exp(jax.random.uniform(key, (count,), jnp.float32, math.log(0.05), math.log(2.0)))
    ramp = jnp.exp(math.log(9.0) * jnp.arange(count, dtype=jnp.float32) / count)
    return jnp.clip(base_value * ramp, 0.05, 18.0)


def draw_acts_in(key, part):
    return scaled_field(jax.random.fold_in(key, 11), TOKENS, D, 1.0)


def draw_grad_query(key, part):
    return scaled_field(jax.random.fold_in(key, 12), TOKENS, Q, 4.0 / math.sqrt(TOKENS))


def draw_attn_out(key, part):
    return scaled_field(jax.random.fold_in(key, 13), TOKENS, Q, 1.0)


def draw_grad_out(key, part):
    return scaled_field(jax.random.fold_in(key, 14), TOKENS, D, 4.0 / math.sqrt(TOKENS))


def draw_row_query(key, part):
    return rising_factor(jax.random.fold_in(key, 15), D)


def draw_row_output(key, part):
    return rising_factor(jax.random.fold_in(key, 16), Q)


def levels(rng, shape, shards, low, top_value):
    loudness = 1.0
    for dim, blocks in shards:
        heights = jax.random.uniform(jax.random.fold_in(jax.random.fold_in(rng, 6), dim), (blocks,), jnp.float32, low / len(shards), top_value / len(shards))
        loudness = loudness * jnp.repeat(jnp.exp(heights), shape[dim] // blocks).reshape((-1,) + (1,) * (len(shape) - 1 - dim))
    return loudness


def setup_inputs(seed: int = 0) -> dict:
    seeds = jax.random.split(jax.random.key(seed), 9)
    acts_in = draw_acts_in(jax.random.fold_in(seeds[8], 71), 0)
    grad_query = draw_grad_query(jax.random.fold_in(seeds[8], 71), 0)
    attn_out = draw_attn_out(jax.random.fold_in(seeds[8], 71), 0)
    grad_out = draw_grad_out(jax.random.fold_in(seeds[8], 71), 0)
    row_query = draw_row_query(jax.random.fold_in(seeds[8], 71), 0)
    col_query = jnp.clip(jnp.exp(math.log(2.0) - 3.6888794 * jax.random.uniform(seeds[5], (Q,), jnp.float32) ** levels(seeds[5], (Q,), ((0, 4),), -0.2, 0.2)), 0.05, 2.0)
    row_output = draw_row_output(jax.random.fold_in(seeds[8], 71), 0)
    col_output = jnp.clip(jnp.exp(math.log(2.0) - 3.6888794 * jax.random.uniform(seeds[7], (D,), jnp.float32) ** levels(seeds[7], (D,), ((0, 4),), -0.2, 0.2)), 0.05, 2.0)
    return dict(acts_in=acts_in, grad_query=grad_query, attn_out=attn_out, grad_out=grad_out, row_query=row_query, col_query=col_query, row_output=row_output, col_output=col_output)


decay_rate = 0.81
epsilon_one = 1e-30

def grouped_gradient(left, right):
    left_groups = left.astype(jnp.float32).reshape(N_ROW, TOK_DEV, left.shape[1])
    right_groups = right.astype(jnp.float32).reshape(N_ROW, TOK_DEV, right.shape[1])

    def add_group(running, paired):
        partial_grad = jnp.dot(paired[0].T, paired[1], precision=lax.Precision.HIGHEST, preferred_element_type=jnp.float32)
        rounded = lax.optimization_barrier(partial_grad.astype(jnp.bfloat16))
        return (running + rounded.astype(jnp.float32), None)
    initial = jnp.zeros((left.shape[1], right.shape[1]), jnp.float32)
    summed, unused = lax.scan(add_group, initial, (left_groups, right_groups))
    return summed

def factored_update(gradient, clip_scale, row_old, col_old):
    clipped = clip_scale * gradient
    squared = clipped * clipped + epsilon_one
    row_new = decay_rate * row_old + (1.0 - decay_rate) * lax.optimization_barrier(jnp.mean(squared, axis=1))
    col_new = decay_rate * col_old + (1.0 - decay_rate) * lax.optimization_barrier(jnp.mean(squared, axis=0))
    row_level = jnp.mean(row_new)
    update = clipped * lax.rsqrt(row_new[:, None] * col_new[None, :] / row_level)
    return (update.astype(jnp.bfloat16), row_new, col_new)

def reference(acts_in, grad_query, attn_out, grad_out, row_query, col_query, row_output, col_output):
    query_grad = grouped_gradient(acts_in, grad_query)
    output_grad = grouped_gradient(attn_out, grad_out)
    grad_norm = jnp.sqrt(jnp.sum(query_grad * query_grad) + jnp.sum(output_grad * output_grad))
    clip_scale = CLIP / jnp.maximum(grad_norm, jnp.float32(CLIP))
    update_query, new_row_query, new_col_query = factored_update(query_grad, clip_scale, row_query, col_query)
    update_output, new_row_output, new_col_output = factored_update(output_grad, clip_scale, row_output, col_output)
    return (update_query, update_output, new_row_query, new_col_query, new_row_output, new_col_output)
```

```python
import functools
import math

import jax
import jax.numpy as jnp
from jax import lax
from jax.experimental import pallas as pl
from jax.experimental.pallas import tpu as pltpu
from jax.sharding import PartitionSpec as P

CLIP = 3072
MESH = pl.DeviceIdType.MESH
LANES = 128

decay_rate = 0.81
epsilon_one = 1e-30


def round_up(value, step):
    return (value + step - 1) // step * step


class Plan:
    def __init__(self, total_rows, cols, n, tokens):
        self.rows = total_rows // n
        self.cols = cols
        self.tokens = tokens
        self.total_rows = total_rows
        self.window = round_up(self.rows + LANES - math.gcd(self.rows, LANES), LANES)
        tiles = cols // LANES
        self.width = LANES * max(t for t in (1, 2, 3) if tiles % t == 0)
        self.pieces = cols // self.width
        self.tile = max(t for t in (64, 48, 32, 16) if self.rows % t == 0)
        self.padded = round_up(self.rows, LANES)


def ring_row(pos, n):
    upper = pos // (n // 2)
    return (1 - upper) * (2 * pos) + upper * (2 * (n - 1 - pos) + 1)


def ring_pos(row, n):
    odd = row % 2
    return (1 - odd) * (row // 2) + odd * (n - 1 - row // 2)


def kernel(
    n, m, plans, lefts_q, rights_q, lefts_o, rights_o, vec_in,
    upd_q, upd_o, vec_out,
    right_q, right_o, win_q, win_o, lt_q, lt_o, part_q, part_o, first_q, first_o, ring_q, ring_o,
    rowacc_q, rowacc_o, packet1, inbox1, packet2, inbox2, scale_q, scale_o,
    load_sem, win_sem, send_q, recv_q, send_o, recv_o, psend1, precv1, psend2, precv2,
):
    row = lax.axis_index("row")
    col = lax.axis_index("col")
    pos = ring_pos(row, n)
    after = ring_row((pos + 1) % n, n)
    before = ring_row((pos + n - 1) % n, n)
    lefts = (lefts_q, lefts_o)
    rights = (right_q, right_o)
    wins = (win_q, win_o)
    lts = (lt_q, lt_o)
    parts = (part_q, part_o)
    firsts = (first_q, first_o)
    rings = (ring_q, ring_o)
    rowaccs = (rowacc_q, rowacc_o)
    scales = (scale_q, scale_o)
    upds = (upd_q, upd_o)
    sends = (send_q, send_o)
    recvs = (recv_q, recv_o)
    target = (after, before)

    loads = [
        pltpu.make_async_copy(rights_q, right_q, load_sem.at[0]),
        pltpu.make_async_copy(rights_o, right_o, load_sem.at[1]),
    ]

    def chunk_of(d, s):
        place = (pos - 1 - s + 2 * n) % n if d == 0 else (pos + 1 + s) % n
        return ring_row(place, n)

    def window_copy(d, s):
        plan = plans[d]
        start = chunk_of(d, s) * plan.rows // LANES * LANES
        return pltpu.make_async_copy(
            lefts[d].at[:, pl.ds(pl.multiple_of(start, LANES), plan.window)],
            wins[d].at[s % 2],
            win_sem.at[d, s % 2],
        )

    def offset_of(d, s):
        plan = plans[d]
        return pl.multiple_of(chunk_of(d, s) * plan.rows % LANES, math.gcd(plan.rows, LANES))

    def hop(d, k, s, src):
        return pltpu.make_async_remote_copy(
            src_ref=src,
            dst_ref=rings[d].at[s, k],
            send_sem=sends[d].at[s, k],
            recv_sem=recvs[d].at[s, k],
            device_id={"row": target[d]},
            device_id_type=MESH,
        )

    def turn(d, s):
        lts[d][...] = wins[d][s % 2].T

    def multiply(d, k):
        plan = plans[d]
        parts[d][k] = jnp.dot(
            lts[d][...],
            rights[d][:, pl.ds(k * plan.width, plan.width)],
            preferred_element_type=jnp.float32,
        )

    for d in range(2):
        loads[d].start()
        window_copy(d, 0).start()
    for d in range(2):
        window_copy(d, 1).start()

    barrier = pltpu.get_barrier_semaphore()
    for step in range(1, n):
        pl.semaphore_signal(barrier, inc=1, device_id={"row": (row + step) % n}, device_id_type=MESH)
    for step in range(1, m):
        pl.semaphore_signal(barrier, inc=1, device_id={"col": (col + step) % m}, device_id_type=MESH)

    def merge(d, k, s, add):
        plan = plans[d]
        off = offset_of(d, s)

        @pl.loop(0, plan.rows // plan.tile)
        def _(t):
            at = pl.multiple_of(t * plan.tile, plan.tile)
            own = parts[d][k, pl.ds(pl.multiple_of(off + at, 16), plan.tile), :]
            if add:
                own = own + rings[d][s - 1, k, pl.ds(at, plan.tile), :].astype(jnp.float32)
                rings[d][s - 1, k, pl.ds(at, plan.tile), :] = own.astype(jnp.bfloat16)
            else:
                firsts[d][k, pl.ds(at, plan.tile), :] = own.astype(jnp.bfloat16)

    order = sorted(
        [(k / plans[d].pieces, d, k) for d in range(2) for k in range(plans[d].pieces)]
    )
    order = [(d, k) for _, d, k in order]

    for d in range(2):
        loads[d].wait()
        window_copy(d, 0).wait()
        turn(d, 0)
    for i, (d, k) in enumerate(order):
        multiply(d, k)
        merge(d, k, 0, False)
        if i == 0:
            pl.semaphore_wait(barrier, n - 1 + m - 1)
        hop(d, k, 0, firsts[d].at[k]).start()

    @pl.loop(1, n - 1)
    def _(s):
        for d in range(2):
            window_copy(d, s).wait()
            turn(d, s)
            window_copy(d, s + 1).start()
            for k in range(plans[d].pieces):
                multiply(d, k)
        for d, k in order:
            hop(d, k, s - 1, rings[d].at[s - 1, k]).wait_recv()
            merge(d, k, s, True)
            hop(d, k, s, rings[d].at[s - 1, k]).start()

    last = n - 1
    for d in range(2):
        window_copy(d, last).wait()
        turn(d, last)
        for k in range(plans[d].pieces):
            multiply(d, k)

    width1 = plans[0].padded
    col_start = (0, plans[0].cols)
    for d in range(2):
        rowaccs[d][...] = jnp.zeros_like(rowaccs[d])
    for d, k in order:
        plan = plans[d]
        hop(d, k, last - 1, rings[d].at[last - 1, k]).wait_recv()
        off = offset_of(d, last)

        def gather(t, sums, d=d, k=k, plan=plan, off=off):
            at = pl.multiple_of(t * plan.tile, plan.tile)
            where = pl.ds(pl.multiple_of(off + at, 16), plan.tile)
            value = parts[d][k, where, :] + rings[d][last - 1, k, pl.ds(at, plan.tile), :].astype(
                jnp.float32
            )
            parts[d][k, where, :] = value
            square = value * value
            across = square[:, :LANES]
            for j in range(1, plan.width // LANES):
                across = across + square[:, j * LANES : (j + 1) * LANES]
            rowaccs[d][pl.ds(at, plan.tile), :] += across
            down = square[:8]
            for j in range(1, plan.tile // 8):
                down = down + square[j * 8 : (j + 1) * 8]
            return sums + down

        sums = lax.fori_loop(0, plan.rows // plan.tile, gather, jnp.zeros((8, plan.width), jnp.float32))
        packet2[:, pl.ds(col_start[d] + k * plan.width, plan.width)] = jnp.sum(
            sums, axis=0, keepdims=True
        )

    row_start = (0, width1)
    for d in range(2):
        packet1[:, pl.ds(row_start[d], plans[d].padded)] = jnp.sum(
            rowaccs[d][...].T, axis=0, keepdims=True
        )

    def share(axis, me, count, packet, inbox, ssem, rsem):
        copies = []
        for step in range(1, count):
            copies.append(
                pltpu.make_async_remote_copy(
                    src_ref=packet,
                    dst_ref=inbox.at[step - 1],
                    send_sem=ssem.at[step - 1],
                    recv_sem=rsem.at[step - 1],
                    device_id={axis: (me + step) % count},
                    device_id_type=MESH,
                )
            )
            copies[-1].start()
        total = packet[...]
        for step in range(1, count):
            copies[step - 1].wait_recv()
            total = total + inbox[step - 1]
        return total, copies

    row_total, copies1 = share("col", col, m, packet1, inbox1, psend1, precv1)
    row_sums = [row_total[:, row_start[d] : row_start[d] + plans[d].padded] for d in range(2)]
    row_old = [vec_in[:, pl.ds(row_start[d], plans[d].padded)] for d in range(2)]
    vec_col = width1 + plans[1].padded
    lane = lax.broadcasted_iota(jnp.int32, (1, LANES), 1)
    scalars = jnp.zeros((1, LANES), jnp.float32)
    for i, value in enumerate(row_sums + row_old):
        scalars = scalars + jnp.where(lane == i, jnp.sum(value, axis=1, keepdims=True), 0.0)
    all_cols = plans[0].cols + plans[1].cols
    packet2[:, pl.ds(all_cols, LANES)] = scalars
    col_total, copies2 = share("row", row, n, packet2, inbox2, psend2, precv2)
    tail = col_total[:, all_cols : all_cols + LANES]
    squares_q, squares_o, oldsum_q, oldsum_o = [
        jnp.sum(jnp.where(lane == i, tail, 0.0), axis=1, keepdims=True) for i in range(4)
    ]
    clip_scale = CLIP / jnp.maximum(jnp.sqrt(squares_q + squares_o), jnp.float32(CLIP))
    squared_scale = clip_scale * clip_scale
    squares = (squares_q, squares_o)
    oldsums = (oldsum_q, oldsum_o)
    for d in range(2):
        plan = plans[d]
        whole_cols = plan.cols * m
        level = decay_rate * oldsums[d] / plan.total_rows + (1.0 - decay_rate) * (
            squared_scale * squares[d] / (plan.total_rows * whole_cols) + epsilon_one
        )
        new_row = decay_rate * row_old[d] + (1.0 - decay_rate) * (
            squared_scale * row_sums[d] / whole_cols + epsilon_one
        )
        vec_out[:, pl.ds(row_start[d], plan.padded)] = new_row
        cols_at = pl.ds(vec_col + col_start[d], plan.cols)
        new_col = decay_rate * vec_in[:, cols_at] + (1.0 - decay_rate) * (
            squared_scale * col_total[:, col_start[d] : col_start[d] + plan.cols] / plan.total_rows
            + epsilon_one
        )
        vec_out[:, cols_at] = new_col
        across = clip_scale * lax.rsqrt(new_row / level)
        scales[d][...] = jnp.broadcast_to(across, (LANES, plan.padded)).T
        down = lax.rsqrt(new_col)
        off = offset_of(d, last)
        for k in range(plan.pieces):
            here = down[:, k * plan.width : (k + 1) * plan.width]

            @pl.loop(0, plan.rows // plan.tile)
            def _(t, d=d, k=k, plan=plan, off=off, here=here):
                at = pl.multiple_of(t * plan.tile, plan.tile)
                value = parts[d][k, pl.ds(pl.multiple_of(off + at, 16), plan.tile), :]
                factor = scales[d][pl.ds(at, plan.tile), :]
                factor = jnp.concatenate([factor] * (plan.width // LANES), axis=1)
                upds[d][pl.ds(at, plan.tile), pl.ds(k * plan.width, plan.width)] = (
                    value * factor * here
                ).astype(jnp.bfloat16)

    for copy in copies1 + copies2:
        copy.wait_send()

    for d, k in order:
        hop(d, k, 0, firsts[d].at[k]).wait_send()

    @pl.loop(1, n - 1)
    def _(s):
        for d, k in order:
            hop(d, k, s, rings[d].at[s - 1, k]).wait_send()


def shards(n, m, acts_in, grad_query, attn_out, grad_out, row_query, col_query, row_output, col_output):
    bf16, f32 = jnp.bfloat16, jnp.float32
    tokens = acts_in.shape[0]
    plans = (
        Plan(acts_in.shape[1], grad_query.shape[1], n, tokens),
        Plan(attn_out.shape[1], grad_out.shape[1], n, tokens),
    )
    a, b = plans
    vec = jnp.concatenate(
        [
            jnp.pad(row_query, (0, a.padded - a.rows)),
            jnp.pad(row_output, (0, b.padded - b.rows)),
            col_query,
            col_output,
        ]
    )[None, :]
    width = vec.shape[1]
    packet1 = a.padded + b.padded
    packet2 = a.cols + b.cols + LANES
    dma = pltpu.SemaphoreType.DMA
    vmem = pl.BlockSpec(memory_space=pltpu.VMEM)
    hbm = pl.BlockSpec(memory_space=pl.ANY)

    def each(make):
        return [make(a), make(b)]

    update_query, update_output, vec = pl.pallas_call(
        functools.partial(kernel, n, m, plans),
        out_shape=[
            jax.ShapeDtypeStruct((a.rows, a.cols), bf16),
            jax.ShapeDtypeStruct((b.rows, b.cols), bf16),
            jax.ShapeDtypeStruct((1, width), f32),
        ],
        in_specs=[hbm] * 4 + [vmem],
        out_specs=[vmem] * 3,
        scratch_shapes=[
            *each(lambda p: pltpu.VMEM((tokens, p.cols), bf16)),
            *each(lambda p: pltpu.VMEM((2, tokens, p.window), bf16)),
            *each(lambda p: pltpu.VMEM((p.window, tokens), bf16)),
            *each(lambda p: pltpu.VMEM((p.pieces, p.window, p.width), f32)),
            *each(lambda p: pltpu.VMEM((p.pieces, p.rows, p.width), bf16)),
            *each(lambda p: pltpu.VMEM((n - 1, p.pieces, p.rows, p.width), bf16)),
            *each(lambda p: pltpu.VMEM((p.padded, LANES), f32)),
            pltpu.VMEM((1, packet1), f32),
            pltpu.VMEM((m - 1, 1, packet1), f32),
            pltpu.VMEM((1, packet2), f32),
            pltpu.VMEM((n - 1, 1, packet2), f32),
            *each(lambda p: pltpu.VMEM((p.padded, LANES), f32)),
            dma((2,)),
            dma((2, 2)),
            dma((n - 1, a.pieces)),
            dma((n - 1, a.pieces)),
            dma((n - 1, b.pieces)),
            dma((n - 1, b.pieces)),
            dma((m - 1,)),
            dma((m - 1,)),
            dma((n - 1,)),
            dma((n - 1,)),
        ],
        compiler_params=pltpu.CompilerParams(
            collective_id=0, has_side_effects=True, vmem_limit_bytes=64000 * 1024
        ),
    )(acts_in, grad_query, attn_out, grad_out, vec)
    vec = vec[0]
    start = a.padded + b.padded
    return (
        update_query,
        update_output,
        vec[: a.rows],
        vec[start : start + a.cols],
        vec[a.padded : a.padded + b.rows],
        vec[start + a.cols :],
    )


def solution(mesh):
    in_specs = (
        P("row", None),
        P("row", "col"),
        P("row", None),
        P("row", "col"),
        P("row"),
        P("col"),
        P("row"),
        P("col"),
    )
    out_specs = (P("row", "col"), P("row", "col"), P("row"), P("col"), P("row"), P("col"))
    body = functools.partial(shards, mesh.shape["row"], mesh.shape["col"])
    return jax.shard_map(body, mesh=mesh, in_specs=in_specs, out_specs=out_specs, check_vma=False)
```

```python
import functools
import math

import jax
import jax.numpy as jnp
from jax import lax
from jax.experimental import pallas as pl
from jax.experimental.pallas import tpu as pltpu
from jax.sharding import PartitionSpec as P

CLIP = 3072
MESH = pl.DeviceIdType.MESH
LANES = 128

decay_rate = 0.81
epsilon_one = 1e-30


def round_up(value, step):
    return (value + step - 1) // step * step


class Plan:
    def __init__(self, total_rows, cols, n, tokens):
        self.rows = total_rows // n
        self.cols = cols
        self.tokens = tokens
        self.total_rows = total_rows
        self.window = round_up(self.rows + LANES - math.gcd(self.rows, LANES), LANES)
        tiles = cols // LANES
        self.width = LANES * max(t for t in (1, 2, 3) if tiles % t == 0)
        self.pieces = cols // self.width
        self.tile = max(t for t in (64, 48, 32, 16) if self.rows % t == 0)
        self.padded = round_up(self.rows, LANES)
        self.parts = max(p for p in (1, 2, 3, 4) if self.rows % (16 * p) == 0)


def ring_row(pos, n):
    upper = pos // (n // 2)
    return (1 - upper) * (2 * pos) + upper * (2 * (n - 1 - pos) + 1)


def ring_pos(row, n):
    odd = row % 2
    return (1 - odd) * (row // 2) + odd * (n - 1 - row // 2)


def kernel(
    n, m, plans, lefts_q, rights_q, lefts_o, rights_o, old_row_q, old_row_o, old_col_q, old_col_o,
    upd_q, upd_o, vec_out,
    right_q, right_o, win_q, win_o, lt_q, lt_o, part_q, part_o, first_q, first_o, ring_q, ring_o,
    rowacc_q, rowacc_o, packet1, inbox1, packet2, inbox2, packet3, inbox3, scale_q, scale_o,
    load_sem, win_sem, send_q, recv_q, send_o, recv_o, psend1, precv1, psend2, precv2, psend3, precv3,
):
    row = lax.axis_index("row")
    col = lax.axis_index("col")
    pos = ring_pos(row, n)
    after = ring_row((pos + 1) % n, n)
    before = ring_row((pos + n - 1) % n, n)
    lefts = (lefts_q, lefts_o)
    rights = (right_q, right_o)
    wins = (win_q, win_o)
    lts = (lt_q, lt_o)
    parts = (part_q, part_o)
    firsts = (first_q, first_o)
    rings = (ring_q, ring_o)
    rowaccs = (rowacc_q, rowacc_o)
    scales = (scale_q, scale_o)
    upds = (upd_q, upd_o)
    sends = (send_q, send_o)
    recvs = (recv_q, recv_o)
    target = (after, before)

    def load(d, k):
        columns = pl.ds(k * plans[d].width, plans[d].width)
        source = (rights_q, rights_o)[d]
        return pltpu.make_async_copy(
            source.at[:, columns], rights[d].at[:, columns], load_sem.at[d, k]
        )

    def chunk_of(d, s):
        place = (pos - 1 - s + 2 * n) % n if d == 0 else (pos + 1 + s) % n
        return ring_row(place, n)

    def window_copy(d, s):
        plan = plans[d]
        start = chunk_of(d, s) * plan.rows // LANES * LANES
        return pltpu.make_async_copy(
            lefts[d].at[:, pl.ds(pl.multiple_of(start, LANES), plan.window)],
            wins[d].at[s % 2],
            win_sem.at[d, s % 2],
        )

    def offset_of(d, s):
        plan = plans[d]
        return pl.multiple_of(chunk_of(d, s) * plan.rows % LANES, math.gcd(plan.rows, LANES))

    def hop(d, k, s, src):
        return pltpu.make_async_remote_copy(
            src_ref=src,
            dst_ref=rings[d].at[s, k],
            send_sem=sends[d].at[s, k],
            recv_sem=recvs[d].at[s, k],
            device_id={"row": target[d]},
            device_id_type=MESH,
        )

    def turn(d, s):
        lts[d][...] = wins[d][s % 2].T

    def multiply(d, k):
        plan = plans[d]
        parts[d][k] = jnp.dot(
            lts[d][...],
            rights[d][:, pl.ds(k * plan.width, plan.width)],
            preferred_element_type=jnp.float32,
        )

    barrier = pltpu.get_barrier_semaphore()
    for step in range(1, n):
        pl.semaphore_signal(barrier, inc=1, device_id={"row": (row + step) % n}, device_id_type=MESH)
    for step in range(1, m):
        pl.semaphore_signal(barrier, inc=1, device_id={"col": (col + step) % m}, device_id_type=MESH)

    order = sorted(
        [(k / plans[d].pieces, d, k) for d in range(2) for k in range(plans[d].pieces)]
    )
    order = [(d, k) for _, d, k in order]
    for d, k in order:
        if k == 0:
            window_copy(d, 0).start()
        load(d, k).start()

    def merge(d, k, s, add):
        plan = plans[d]
        off = offset_of(d, s)

        @pl.loop(0, plan.rows // plan.tile)
        def _(t):
            at = pl.multiple_of(t * plan.tile, plan.tile)
            own = parts[d][k, pl.ds(pl.multiple_of(off + at, 16), plan.tile), :]
            if add:
                own = own + rings[d][s - 1, k, pl.ds(at, plan.tile), :].astype(jnp.float32)
                rings[d][s - 1, k, pl.ds(at, plan.tile), :] = own.astype(jnp.bfloat16)
            else:
                firsts[d][k, pl.ds(at, plan.tile), :] = own.astype(jnp.bfloat16)

    for i, (d, k) in enumerate(order):
        if k == 0:
            window_copy(d, 0).wait()
            turn(d, 0)
        load(d, k).wait()
        multiply(d, k)
        merge(d, k, 0, False)
        if i == 0:
            pl.semaphore_wait(barrier, n - 1 + m - 1)
        hop(d, k, 0, firsts[d].at[k]).start()
        if k == 0:
            window_copy(d, 1).start()

    @pl.loop(1, n - 1)
    def _(s):
        for d in range(2):
            window_copy(d, s).wait()
            turn(d, s)
            window_copy(d, s + 1).start()
            for k in range(plans[d].pieces):
                multiply(d, k)
        for d, k in order:
            hop(d, k, s - 1, rings[d].at[s - 1, k]).wait_recv()
            merge(d, k, s, True)
            hop(d, k, s, rings[d].at[s - 1, k]).start()

    last = n - 1
    for d in range(2):
        window_copy(d, last).wait()
        turn(d, last)
        for k in range(plans[d].pieces):
            multiply(d, k)

    width1 = plans[0].padded
    col_start = (0, plans[0].cols)
    for d in range(2):
        rowaccs[d][...] = jnp.zeros_like(rowaccs[d])
    for d, k in order:
        plan = plans[d]
        hop(d, k, last - 1, rings[d].at[last - 1, k]).wait_recv()
        off = offset_of(d, last)

        def gather(t, sums, d=d, k=k, plan=plan, off=off):
            at = pl.multiple_of(t * plan.tile, plan.tile)
            where = pl.ds(pl.multiple_of(off + at, 16), plan.tile)
            value = parts[d][k, where, :] + rings[d][last - 1, k, pl.ds(at, plan.tile), :].astype(
                jnp.float32
            )
            parts[d][k, where, :] = value
            square = value * value
            across = square[:, :LANES]
            for j in range(1, plan.width // LANES):
                across = across + square[:, j * LANES : (j + 1) * LANES]
            rowaccs[d][pl.ds(at, plan.tile), :] += across
            down = square[:8]
            for j in range(1, plan.tile // 8):
                down = down + square[j * 8 : (j + 1) * 8]
            return sums + down

        sums = lax.fori_loop(0, plan.rows // plan.tile, gather, jnp.zeros((8, plan.width), jnp.float32))
        packet2[:, pl.ds(col_start[d] + k * plan.width, plan.width)] = jnp.sum(
            sums, axis=0, keepdims=True
        )

    row_start = (0, width1)
    for d in range(2):
        packet1[:, pl.ds(row_start[d], plans[d].padded)] = jnp.sum(
            rowaccs[d][...].T, axis=0, keepdims=True
        )

    def share(axis, me, count, packet, inbox, ssem, rsem):
        copies = []
        for step in range(1, count):
            copies.append(
                pltpu.make_async_remote_copy(
                    src_ref=packet,
                    dst_ref=inbox.at[step - 1],
                    send_sem=ssem.at[step - 1],
                    recv_sem=rsem.at[step - 1],
                    device_id={axis: (me + step) % count},
                    device_id_type=MESH,
                )
            )
            copies[-1].start()
        return copies

    def total_of(copies, packet, inbox):
        total = packet[...]
        for i, copy in enumerate(copies):
            copy.wait_recv()
            total = total + inbox[i]
        return total

    copies1 = share("col", col, m, packet1, inbox1, psend1, precv1)
    copies2 = share("row", row, n, packet2, inbox2, psend2, precv2)
    row_total = total_of(copies1, packet1, inbox1)
    row_sums = [row_total[:, row_start[d] : row_start[d] + plans[d].padded] for d in range(2)]
    row_old = [
        jnp.pad(ref[...][None, :], ((0, 0), (0, plans[d].padded - plans[d].rows)))
        for d, ref in enumerate((old_row_q, old_row_o))
    ]
    vec_col = width1 + plans[1].padded
    lane = lax.broadcasted_iota(jnp.int32, (1, LANES), 1)
    scalars = jnp.zeros((1, LANES), jnp.float32)
    for i, value in enumerate(row_sums + row_old):
        scalars = scalars + jnp.where(lane == i, jnp.sum(value, axis=1, keepdims=True), 0.0)
    packet3[...] = scalars
    copies3 = share("row", row, n, packet3, inbox3, psend3, precv3)
    col_total = total_of(copies2, packet2, inbox2)
    tail = total_of(copies3, packet3, inbox3)
    squares_q, squares_o, oldsum_q, oldsum_o = [
        jnp.sum(jnp.where(lane == i, tail, 0.0), axis=1, keepdims=True) for i in range(4)
    ]
    clip_scale = CLIP / jnp.maximum(jnp.sqrt(squares_q + squares_o), jnp.float32(CLIP))
    squared_scale = clip_scale * clip_scale
    squares = (squares_q, squares_o)
    oldsums = (oldsum_q, oldsum_o)
    for d in range(2):
        plan = plans[d]
        whole_cols = plan.cols * m
        level = decay_rate * oldsums[d] / plan.total_rows + (1.0 - decay_rate) * (
            squared_scale * squares[d] / (plan.total_rows * whole_cols) + epsilon_one
        )
        new_row = decay_rate * row_old[d] + (1.0 - decay_rate) * (
            squared_scale * row_sums[d] / whole_cols + epsilon_one
        )
        vec_out[:, pl.ds(row_start[d], plan.padded)] = new_row
        cols_at = pl.ds(vec_col + col_start[d], plan.cols)
        new_col = decay_rate * (old_col_q, old_col_o)[d][...][None, :] + (1.0 - decay_rate) * (
            squared_scale * col_total[:, col_start[d] : col_start[d] + plan.cols] / plan.total_rows
            + epsilon_one
        )
        vec_out[:, cols_at] = new_col
        across = clip_scale * lax.rsqrt(new_row / level)
        scales[d][...] = jnp.broadcast_to(across, (LANES, plan.padded)).T
        down = lax.rsqrt(new_col)
        off = offset_of(d, last)
        for k in range(plan.pieces):
            here = down[:, k * plan.width : (k + 1) * plan.width]

            @pl.loop(0, plan.rows // plan.tile)
            def _(t, d=d, k=k, plan=plan, off=off, here=here):
                at = pl.multiple_of(t * plan.tile, plan.tile)
                value = parts[d][k, pl.ds(pl.multiple_of(off + at, 16), plan.tile), :]
                factor = scales[d][pl.ds(at, plan.tile), :]
                factor = jnp.concatenate([factor] * (plan.width // LANES), axis=1)
                upds[d][pl.ds(at, plan.tile), pl.ds(k * plan.width, plan.width)] = (
                    value * factor * here
                ).astype(jnp.bfloat16)

    for copy in copies1 + copies2 + copies3:
        copy.wait_send()

    for d, k in order:
        hop(d, k, 0, firsts[d].at[k]).wait_send()

    @pl.loop(1, n - 1)
    def _(s):
        for d, k in order:
            hop(d, k, s, rings[d].at[s - 1, k]).wait_send()


def deliver(plans, in_q, in_o, vec, upd_q, upd_o, row_q, col_q, row_o, col_o, hold_q, hold_o, sem):
    a, b = plans

    def copy(d, i, out):
        size = plans[d].rows // plans[d].parts
        part = pl.ds(i * size, size)
        hold = (hold_q, hold_o)[d].at[part]
        source = (in_q, in_o)[d].at[part]
        result = (upd_q, upd_o)[d].at[part]
        if out:
            return pltpu.make_async_copy(hold, result, sem.at[d, out, i])
        return pltpu.make_async_copy(source, hold, sem.at[d, out, i])

    every = [(d, i) for d in range(2) for i in range(plans[d].parts)]
    for d, i in every:
        copy(d, i, 0).start()
    start = 0
    for ref, size, padded in (
        (row_q, a.rows, a.padded),
        (row_o, b.rows, b.padded),
        (col_q, a.cols, a.cols),
        (col_o, b.cols, b.cols),
    ):
        ref[...] = vec[0, pl.ds(start, padded)][:size]
        start += padded
    for d, i in every:
        copy(d, i, 0).wait()
        copy(d, i, 1).start()
    for d, i in every:
        copy(d, i, 1).wait()


def shards(n, m, acts_in, grad_query, attn_out, grad_out, row_query, col_query, row_output, col_output):
    bf16, f32 = jnp.bfloat16, jnp.float32
    tokens = acts_in.shape[0]
    plans = (
        Plan(acts_in.shape[1], grad_query.shape[1], n, tokens),
        Plan(attn_out.shape[1], grad_out.shape[1], n, tokens),
    )
    a, b = plans
    olds = (row_query, row_output, col_query, col_output)
    width = a.padded + b.padded + a.cols + b.cols
    packet1 = a.padded + b.padded
    packet2 = a.cols + b.cols
    dma = pltpu.SemaphoreType.DMA
    vmem = pl.BlockSpec(memory_space=pltpu.VMEM)
    hbm = pl.BlockSpec(memory_space=pl.ANY)

    def each(make):
        return [make(a), make(b)]

    update_query, update_output, vec = pl.pallas_call(
        functools.partial(kernel, n, m, plans),
        out_shape=[
            jax.ShapeDtypeStruct((a.rows, a.cols), bf16),
            jax.ShapeDtypeStruct((b.rows, b.cols), bf16),
            jax.ShapeDtypeStruct((1, width), f32),
        ],
        in_specs=[hbm] * 4 + [vmem] * 4,
        out_specs=[vmem] * 3,
        scratch_shapes=[
            *each(lambda p: pltpu.VMEM((tokens, p.cols), bf16)),
            *each(lambda p: pltpu.VMEM((2, tokens, p.window), bf16)),
            *each(lambda p: pltpu.VMEM((p.window, tokens), bf16)),
            *each(lambda p: pltpu.VMEM((p.pieces, p.window, p.width), f32)),
            *each(lambda p: pltpu.VMEM((p.pieces, p.rows, p.width), bf16)),
            *each(lambda p: pltpu.VMEM((n - 1, p.pieces, p.rows, p.width), bf16)),
            *each(lambda p: pltpu.VMEM((p.padded, LANES), f32)),
            pltpu.VMEM((1, packet1), f32),
            pltpu.VMEM((m - 1, 1, packet1), f32),
            pltpu.VMEM((1, packet2), f32),
            pltpu.VMEM((n - 1, 1, packet2), f32),
            pltpu.VMEM((1, LANES), f32),
            pltpu.VMEM((n - 1, 1, LANES), f32),
            *each(lambda p: pltpu.VMEM((p.padded, LANES), f32)),
            dma((2, max(a.pieces, b.pieces))),
            dma((2, 2)),
            dma((n - 1, a.pieces)),
            dma((n - 1, a.pieces)),
            dma((n - 1, b.pieces)),
            dma((n - 1, b.pieces)),
            dma((m - 1,)),
            dma((m - 1,)),
            dma((n - 1,)),
            dma((n - 1,)),
            dma((n - 1,)),
            dma((n - 1,)),
        ],
        compiler_params=pltpu.CompilerParams(
            collective_id=0, has_side_effects=True, vmem_limit_bytes=64000 * 1024
        ),
    )(acts_in, grad_query, attn_out, grad_out, *olds)
    return pl.pallas_call(
        functools.partial(deliver, plans),
        out_shape=[
            jax.ShapeDtypeStruct((a.rows, a.cols), bf16),
            jax.ShapeDtypeStruct((b.rows, b.cols), bf16),
            jax.ShapeDtypeStruct((a.rows,), f32),
            jax.ShapeDtypeStruct((a.cols,), f32),
            jax.ShapeDtypeStruct((b.rows,), f32),
            jax.ShapeDtypeStruct((b.cols,), f32),
        ],
        in_specs=[hbm, hbm, vmem],
        out_specs=[hbm] * 2 + [vmem] * 4,
        scratch_shapes=[
            *each(lambda p: pltpu.VMEM((p.rows, p.cols), bf16)),
            dma((2, 2, max(a.parts, b.parts))),
        ],
    )(update_query, update_output, vec)


def solution(mesh):
    in_specs = (
        P("row", None),
        P("row", "col"),
        P("row", None),
        P("row", "col"),
        P("row"),
        P("col"),
        P("row"),
        P("col"),
    )
    out_specs = (P("row", "col"), P("row", "col"), P("row"), P("col"), P("row"), P("col"))
    body = functools.partial(shards, mesh.shape["row"], mesh.shape["col"])
    return jax.shard_map(body, mesh=mesh, in_specs=in_specs, out_specs=out_specs, check_vma=False)
```

```python
import functools
import math

import jax
import jax.numpy as jnp
from jax import lax
from jax.experimental import pallas as pl
from jax.experimental.pallas import tpu as pltpu
from jax.sharding import PartitionSpec as P

CLIP = 3072
MESH = pl.DeviceIdType.MESH
LANES = 128

decay_rate = 0.81
epsilon_one = 1e-30


def round_up(value, step):
    return (value + step - 1) // step * step


class Plan:
    def __init__(self, total_rows, cols, n, tokens):
        self.rows = total_rows // n
        self.cols = cols
        self.tokens = tokens
        self.total_rows = total_rows
        self.window = round_up(self.rows + LANES - math.gcd(self.rows, LANES), LANES)
        tiles = cols // LANES
        self.width = LANES * max(t for t in (1, 2, 3) if tiles % t == 0)
        self.pieces = cols // self.width
        self.tile = max(t for t in (64, 48, 32, 16) if self.rows % t == 0)
        self.padded = round_up(self.rows, LANES)
        self.parts = max(p for p in (1, 2, 3, 4) if self.rows % (16 * p) == 0)


def ring_row(pos, n):
    upper = pos // (n // 2)
    return (1 - upper) * (2 * pos) + upper * (2 * (n - 1 - pos) + 1)


def ring_pos(row, n):
    odd = row % 2
    return (1 - odd) * (row // 2) + odd * (n - 1 - row // 2)


def kernel(
    n, m, plans, lefts_q, rights_q, lefts_o, rights_o, old_row_q, old_row_o, old_col_q, old_col_o,
    grad_q, grad_o, vec_out, fac_out,
    right_q, right_o, win_q, win_o, lt_q, lt_o, part_q, part_o, first_q, first_o, ring_q, ring_o,
    rowacc_q, rowacc_o, packet1, inbox1, packet2, inbox2, packet3, inbox3,
    load_sem, win_sem, out_sem, send_q, recv_q, send_o, recv_o, psend1, precv1, psend2, precv2, psend3, precv3,
):
    row = lax.axis_index("row")
    col = lax.axis_index("col")
    pos = ring_pos(row, n)
    after = ring_row((pos + 1) % n, n)
    before = ring_row((pos + n - 1) % n, n)
    lefts = (lefts_q, lefts_o)
    rights = (right_q, right_o)
    wins = (win_q, win_o)
    lts = (lt_q, lt_o)
    parts = (part_q, part_o)
    firsts = (first_q, first_o)
    rings = (ring_q, ring_o)
    rowaccs = (rowacc_q, rowacc_o)
    grads = (grad_q, grad_o)
    sends = (send_q, send_o)
    recvs = (recv_q, recv_o)
    target = (after, before)

    def load(d, k):
        columns = pl.ds(k * plans[d].width, plans[d].width)
        source = (rights_q, rights_o)[d]
        return pltpu.make_async_copy(
            source.at[:, columns], rights[d].at[:, columns], load_sem.at[d, k]
        )

    def chunk_of(d, s):
        place = (pos - 1 - s + 2 * n) % n if d == 0 else (pos + 1 + s) % n
        return ring_row(place, n)

    def window_copy(d, s):
        plan = plans[d]
        start = chunk_of(d, s) * plan.rows // LANES * LANES
        return pltpu.make_async_copy(
            lefts[d].at[:, pl.ds(pl.multiple_of(start, LANES), plan.window)],
            wins[d].at[s % 2],
            win_sem.at[d, s % 2],
        )

    def offset_of(d, s):
        plan = plans[d]
        return pl.multiple_of(chunk_of(d, s) * plan.rows % LANES, math.gcd(plan.rows, LANES))

    def hop(d, k, s, src):
        return pltpu.make_async_remote_copy(
            src_ref=src,
            dst_ref=rings[d].at[s, k],
            send_sem=sends[d].at[s, k],
            recv_sem=recvs[d].at[s, k],
            device_id={"row": target[d]},
            device_id_type=MESH,
        )

    def turn(d, s):
        lts[d][...] = wins[d][s % 2].T

    def multiply(d, k):
        plan = plans[d]
        parts[d][k] = jnp.dot(
            lts[d][...],
            rights[d][:, pl.ds(k * plan.width, plan.width)],
            preferred_element_type=jnp.float32,
        )

    barrier = pltpu.get_barrier_semaphore()
    for step in range(1, n):
        pl.semaphore_signal(barrier, inc=1, device_id={"row": (row + step) % n}, device_id_type=MESH)
    for step in range(1, m):
        pl.semaphore_signal(barrier, inc=1, device_id={"col": (col + step) % m}, device_id_type=MESH)

    order = sorted(
        [(k / plans[d].pieces, d, k) for d in range(2) for k in range(plans[d].pieces)]
    )
    order = [(d, k) for _, d, k in order]
    for d, k in order:
        if k == 0:
            window_copy(d, 0).start()
        load(d, k).start()

    def merge(d, k, s, add):
        plan = plans[d]
        off = offset_of(d, s)

        @pl.loop(0, plan.rows // plan.tile)
        def _(t):
            at = pl.multiple_of(t * plan.tile, plan.tile)
            own = parts[d][k, pl.ds(pl.multiple_of(off + at, 16), plan.tile), :]
            if add:
                own = own + rings[d][s - 1, k, pl.ds(at, plan.tile), :].astype(jnp.float32)
                rings[d][s - 1, k, pl.ds(at, plan.tile), :] = own.astype(jnp.bfloat16)
            else:
                firsts[d][k, pl.ds(at, plan.tile), :] = own.astype(jnp.bfloat16)

    for i, (d, k) in enumerate(order):
        if k == 0:
            window_copy(d, 0).wait()
            turn(d, 0)
        load(d, k).wait()
        multiply(d, k)
        merge(d, k, 0, False)
        if i == 0:
            pl.semaphore_wait(barrier, n - 1 + m - 1)
        hop(d, k, 0, firsts[d].at[k]).start()
        if k == 0:
            window_copy(d, 1).start()

    @pl.loop(1, n - 1)
    def _(s):
        for d in range(2):
            window_copy(d, s).wait()
            turn(d, s)
            window_copy(d, s + 1).start()
            for k in range(plans[d].pieces):
                multiply(d, k)
        for d, k in order:
            hop(d, k, s - 1, rings[d].at[s - 1, k]).wait_recv()
            merge(d, k, s, True)
            hop(d, k, s, rings[d].at[s - 1, k]).start()

    last = n - 1
    for d in range(2):
        window_copy(d, last).wait()
        turn(d, last)
        for k in range(plans[d].pieces):
            multiply(d, k)

    width1 = plans[0].padded
    col_start = (0, plans[0].cols)
    for d in range(2):
        rowaccs[d][...] = jnp.zeros_like(rowaccs[d])

    def leave(d, k):
        plan = plans[d]
        return pltpu.make_async_copy(
            parts[d].at[k, pl.ds(offset_of(d, last), plan.rows), :],
            grads[d].at[:, pl.ds(k * plan.width, plan.width)],
            out_sem.at[d, k],
        )

    for d, k in order:
        plan = plans[d]
        hop(d, k, last - 1, rings[d].at[last - 1, k]).wait_recv()
        off = offset_of(d, last)

        def gather(t, sums, d=d, k=k, plan=plan, off=off):
            at = pl.multiple_of(t * plan.tile, plan.tile)
            where = pl.ds(pl.multiple_of(off + at, 16), plan.tile)
            value = parts[d][k, where, :] + rings[d][last - 1, k, pl.ds(at, plan.tile), :].astype(
                jnp.float32
            )
            parts[d][k, where, :] = value
            square = value * value
            across = square[:, :LANES]
            for j in range(1, plan.width // LANES):
                across = across + square[:, j * LANES : (j + 1) * LANES]
            rowaccs[d][pl.ds(at, plan.tile), :] += across
            down = square[:8]
            for j in range(1, plan.tile // 8):
                down = down + square[j * 8 : (j + 1) * 8]
            return sums + down

        sums = lax.fori_loop(0, plan.rows // plan.tile, gather, jnp.zeros((8, plan.width), jnp.float32))
        packet2[:, pl.ds(col_start[d] + k * plan.width, plan.width)] = jnp.sum(
            sums, axis=0, keepdims=True
        )
        leave(d, k).start()

    row_start = (0, width1)
    for d in range(2):
        packet1[:, pl.ds(row_start[d], plans[d].padded)] = jnp.sum(
            rowaccs[d][...].T, axis=0, keepdims=True
        )

    def share(axis, me, count, packet, inbox, ssem, rsem):
        copies = []
        for step in range(1, count):
            copies.append(
                pltpu.make_async_remote_copy(
                    src_ref=packet,
                    dst_ref=inbox.at[step - 1],
                    send_sem=ssem.at[step - 1],
                    recv_sem=rsem.at[step - 1],
                    device_id={axis: (me + step) % count},
                    device_id_type=MESH,
                )
            )
            copies[-1].start()
        return copies

    def total_of(copies, packet, inbox):
        total = packet[...]
        for i, copy in enumerate(copies):
            copy.wait_recv()
            total = total + inbox[i]
        return total

    copies1 = share("col", col, m, packet1, inbox1, psend1, precv1)
    copies2 = share("row", row, n, packet2, inbox2, psend2, precv2)
    row_total = total_of(copies1, packet1, inbox1)
    row_sums = [row_total[:, row_start[d] : row_start[d] + plans[d].padded] for d in range(2)]
    row_old = [
        jnp.pad(ref[...][None, :], ((0, 0), (0, plans[d].padded - plans[d].rows)))
        for d, ref in enumerate((old_row_q, old_row_o))
    ]
    vec_col = width1 + plans[1].padded
    lane = lax.broadcasted_iota(jnp.int32, (1, LANES), 1)
    scalars = jnp.zeros((1, LANES), jnp.float32)
    for i, value in enumerate(row_sums + row_old):
        scalars = scalars + jnp.where(lane == i, jnp.sum(value, axis=1, keepdims=True), 0.0)
    packet3[...] = scalars
    copies3 = share("row", row, n, packet3, inbox3, psend3, precv3)
    col_total = total_of(copies2, packet2, inbox2)
    tail = total_of(copies3, packet3, inbox3)
    squares_q, squares_o, oldsum_q, oldsum_o = [
        jnp.sum(jnp.where(lane == i, tail, 0.0), axis=1, keepdims=True) for i in range(4)
    ]
    clip_scale = CLIP / jnp.maximum(jnp.sqrt(squares_q + squares_o), jnp.float32(CLIP))
    squared_scale = clip_scale * clip_scale
    squares = (squares_q, squares_o)
    oldsums = (oldsum_q, oldsum_o)
    for d in range(2):
        plan = plans[d]
        whole_cols = plan.cols * m
        level = decay_rate * oldsums[d] / plan.total_rows + (1.0 - decay_rate) * (
            squared_scale * squares[d] / (plan.total_rows * whole_cols) + epsilon_one
        )
        new_row = decay_rate * row_old[d] + (1.0 - decay_rate) * (
            squared_scale * row_sums[d] / whole_cols + epsilon_one
        )
        vec_out[:, pl.ds(row_start[d], plan.padded)] = new_row
        cols_at = pl.ds(vec_col + col_start[d], plan.cols)
        new_col = decay_rate * (old_col_q, old_col_o)[d][...][None, :] + (1.0 - decay_rate) * (
            squared_scale * col_total[:, col_start[d] : col_start[d] + plan.cols] / plan.total_rows
            + epsilon_one
        )
        vec_out[:, cols_at] = new_col
        fac_out[:, pl.ds(row_start[d], plan.padded)] = clip_scale * lax.rsqrt(new_row / level)
        fac_out[:, cols_at] = lax.rsqrt(new_col)

    for d, k in order:
        leave(d, k).wait()
    for copy in copies1 + copies2 + copies3:
        copy.wait_send()

    for d, k in order:
        hop(d, k, 0, firsts[d].at[k]).wait_send()

    @pl.loop(1, n - 1)
    def _(s):
        for d, k in order:
            hop(d, k, s, rings[d].at[s - 1, k]).wait_send()


def deliver(
    plans, in_q, in_o, vec, factors, upd_q, upd_o, row_q, col_q, row_o, col_o,
    grad_q, grad_o, hold_q, hold_o, scale_q, scale_o, sem,
):
    a, b = plans

    def copy(d, i, out):
        size = plans[d].rows // plans[d].parts
        part = pl.ds(i * size, size)
        if out:
            return pltpu.make_async_copy(
                (hold_q, hold_o)[d].at[part], (upd_q, upd_o)[d].at[part], sem.at[d, out, i]
            )
        return pltpu.make_async_copy(
            (in_q, in_o)[d].at[part], (grad_q, grad_o)[d].at[part], sem.at[d, out, i]
        )

    every = [(d, i) for d in range(2) for i in range(plans[d].parts)]
    for d, i in every:
        copy(d, i, 0).start()
    start = 0
    for ref, size, padded in (
        (row_q, a.rows, a.padded),
        (row_o, b.rows, b.padded),
        (col_q, a.cols, a.cols),
        (col_o, b.cols, b.cols),
    ):
        ref[...] = vec[0, pl.ds(start, padded)][:size]
        start += padded
    row_start = (0, a.padded)
    col_start = (a.padded + b.padded, a.padded + b.padded + a.cols)
    scales = (scale_q, scale_o)
    for d in range(2):
        across = factors[:, pl.ds(row_start[d], plans[d].padded)]
        scales[d][...] = jnp.broadcast_to(across, (LANES, plans[d].padded)).T
    for d, i in every:
        plan = plans[d]
        size = plan.rows // plan.parts
        grad, hold = (grad_q, grad_o)[d], (hold_q, hold_o)[d]
        copy(d, i, 0).wait()

        @pl.loop(0, size // 16)
        def _(t, d=d, i=i, plan=plan, size=size, grad=grad, hold=hold):
            rows = pl.ds(pl.multiple_of(i * size + t * 16, 16), 16)
            factor = scales[d][rows, :]
            for j in range(plan.cols // LANES):
                lanes = pl.ds(j * LANES, LANES)
                down = factors[:, pl.ds(col_start[d] + j * LANES, LANES)]
                hold[rows, lanes] = (grad[rows, lanes] * factor * down).astype(jnp.bfloat16)

        copy(d, i, 1).start()
    for d, i in every:
        copy(d, i, 1).wait()


def shards(n, m, acts_in, grad_query, attn_out, grad_out, row_query, col_query, row_output, col_output):
    bf16, f32 = jnp.bfloat16, jnp.float32
    tokens = acts_in.shape[0]
    plans = (
        Plan(acts_in.shape[1], grad_query.shape[1], n, tokens),
        Plan(attn_out.shape[1], grad_out.shape[1], n, tokens),
    )
    a, b = plans
    olds = (row_query, row_output, col_query, col_output)
    width = a.padded + b.padded + a.cols + b.cols
    packet1 = a.padded + b.padded
    packet2 = a.cols + b.cols
    dma = pltpu.SemaphoreType.DMA
    vmem = pl.BlockSpec(memory_space=pltpu.VMEM)
    hbm = pl.BlockSpec(memory_space=pl.ANY)

    def each(make):
        return [make(a), make(b)]

    query_grad, output_grad, vec, factors = pl.pallas_call(
        functools.partial(kernel, n, m, plans),
        out_shape=[
            jax.ShapeDtypeStruct((a.rows, a.cols), f32),
            jax.ShapeDtypeStruct((b.rows, b.cols), f32),
            jax.ShapeDtypeStruct((1, width), f32),
            jax.ShapeDtypeStruct((1, width), f32),
        ],
        in_specs=[hbm] * 4 + [vmem] * 4,
        out_specs=[hbm] * 2 + [vmem] * 2,
        scratch_shapes=[
            *each(lambda p: pltpu.VMEM((tokens, p.cols), bf16)),
            *each(lambda p: pltpu.VMEM((2, tokens, p.window), bf16)),
            *each(lambda p: pltpu.VMEM((p.window, tokens), bf16)),
            *each(lambda p: pltpu.VMEM((p.pieces, p.window, p.width), f32)),
            *each(lambda p: pltpu.VMEM((p.pieces, p.rows, p.width), bf16)),
            *each(lambda p: pltpu.VMEM((n - 1, p.pieces, p.rows, p.width), bf16)),
            *each(lambda p: pltpu.VMEM((p.padded, LANES), f32)),
            pltpu.VMEM((1, packet1), f32),
            pltpu.VMEM((m - 1, 1, packet1), f32),
            pltpu.VMEM((1, packet2), f32),
            pltpu.VMEM((n - 1, 1, packet2), f32),
            pltpu.VMEM((1, LANES), f32),
            pltpu.VMEM((n - 1, 1, LANES), f32),
            dma((2, max(a.pieces, b.pieces))),
            dma((2, 2)),
            dma((2, max(a.pieces, b.pieces))),
            dma((n - 1, a.pieces)),
            dma((n - 1, a.pieces)),
            dma((n - 1, b.pieces)),
            dma((n - 1, b.pieces)),
            dma((m - 1,)),
            dma((m - 1,)),
            dma((n - 1,)),
            dma((n - 1,)),
            dma((n - 1,)),
            dma((n - 1,)),
        ],
        compiler_params=pltpu.CompilerParams(
            collective_id=0, has_side_effects=True, vmem_limit_bytes=64000 * 1024
        ),
    )(acts_in, grad_query, attn_out, grad_out, *olds)
    return pl.pallas_call(
        functools.partial(deliver, plans),
        out_shape=[
            jax.ShapeDtypeStruct((a.rows, a.cols), bf16),
            jax.ShapeDtypeStruct((b.rows, b.cols), bf16),
            jax.ShapeDtypeStruct((a.rows,), f32),
            jax.ShapeDtypeStruct((a.cols,), f32),
            jax.ShapeDtypeStruct((b.rows,), f32),
            jax.ShapeDtypeStruct((b.cols,), f32),
        ],
        in_specs=[hbm, hbm, vmem, vmem],
        out_specs=[hbm] * 2 + [vmem] * 4,
        scratch_shapes=[
            *each(lambda p: pltpu.VMEM((p.rows, p.cols), f32)),
            *each(lambda p: pltpu.VMEM((p.rows, p.cols), bf16)),
            *each(lambda p: pltpu.VMEM((p.padded, LANES), f32)),
            dma((2, 2, max(a.parts, b.parts))),
        ],
    )(query_grad, output_grad, vec, factors)


def solution(mesh):
    in_specs = (
        P("row", None),
        P("row", "col"),
        P("row", None),
        P("row", "col"),
        P("row"),
        P("col"),
        P("row"),
        P("col"),
    )
    out_specs = (P("row", "col"), P("row", "col"), P("row"), P("col"), P("row"), P("col"))
    body = functools.partial(shards, mesh.shape["row"], mesh.shape["col"])
    return jax.shard_map(body, mesh=mesh, in_specs=in_specs, out_specs=out_specs, check_vma=False)
```
